32 devices in a mesh: dp: 16 (over z, x, core), tensor: 2 (over y).
Axes of the slice: x: 2, y: 2, z: 4, core: 2. Of those that a mesh axis runs over, the one named last changes fastest.
Arguments:
- residual: bfloat16 [4096, 4096], P('dp', 'tensor'), may hold values from -6 to 6
- fresh_qkv: bfloat16 [4096, 3, 2048], P('dp', None, 'tensor'), may hold values from -110 to 110
- active: int32 [4096], P('dp'), may hold values from 0 to 1
- home_slot: int32 [4096], P('dp'), may hold values from 0 to 4095, as said below
- kv_cache: bfloat16 [4096, 2, 16, 2048], P('dp', None, None, 'tensor'), may hold values from -6 to 6
- lengths: int32 [4096], P('dp'), may hold values from 2 to 16
- w_out: bfloat16 [2048, 4096], P('tensor'), may hold values from -0.125 to 0.125
Outputs:
- updated: bfloat16 [4096, 4096], P('dp', 'tensor')
The draws below stay inside these ranges and needn't reach their ends.
Inputs may be any that keep to these rules, and one draw needn't show every extreme that they name: Each dp group owns the slots 256 * g to 256 * g + 255; home_slot is a permutation. Among the streams of one dp group, at most 16 active streams have slots in the same owning group, and this is reached in every draw.
All inputs are finite; a program needn't handle non-finite values.
Results may differ from the reference program's by a relative error of at most 0.0062.
Values may be sent and summed in bfloat16 or wider, within the bound.
A program may use at most 128 MiB of HBM per device.

```python
import jax
import jax.numpy as jnp
from jax import lax

D = 4096
HEADS = 16
HD = 128
S_DEV = 256
L = 16
CAP = 16
STREAMS = 4096


def routing(key):
    base = jax.random.fold_in(key, 101)
    groups = STREAMS // S_DEV
    stream_index = jnp.arange(STREAMS, dtype=jnp.int32)
    source = stream_index // S_DEV
    within = stream_index % S_DEV
    shuffled = jax.random.permutation(jax.random.fold_in(base, 1), groups).astype(jnp.int32)
    inverse = jnp.argsort(shuffled).astype(jnp.int32)
    values = jnp.arange(groups, dtype=jnp.int32)
    priority = jnp.where(values == 1, 0, jnp.where(values == groups - 1, 1, jnp.where(values == groups // 2, 2, 3 + inverse)))
    offsets = jnp.argsort(priority).astype(jnp.int32)[:S_DEV // CAP]
    owner_group = (source + offsets[within // CAP]) % groups
    ranking = jax.random.randint(jax.random.fold_in(base, 2), (groups, S_DEV), 0, 1 << 20) * S_DEV + jnp.arange(S_DEV, dtype=jnp.int32)[None, :]
    slot_order = jnp.argsort(ranking, axis=1).astype(jnp.int32)
    home_slot = owner_group * S_DEV + slot_order[owner_group, within]
    active_level = jax.random.randint(jax.random.fold_in(base, 3), (groups,), 2, 9)
    dice_roll = jax.random.randint(jax.random.fold_in(base, 4), (STREAMS,), 0, 8)
    active = jnp.logical_or(dice_roll < active_level[owner_group], stream_index < CAP)
    return (home_slot.astype(jnp.int32), active.astype(jnp.int32))


def draw_home_slot(key, part):
    return routing(key)[0]


def draw_active(key, part):
    return routing(key)[1]


def draw_fresh_qkv(key, part):
    drawn = jnp.clip(jax.random.normal(jax.random.fold_in(key, 201), (STREAMS, 3, HEADS * HD), jnp.float32), -6.0, 6.0)
    return drawn.astype(jnp.bfloat16)


def draw_kv_cache(key, part):
    drawn = jnp.clip(jax.random.normal(jax.random.fold_in(key, 202), (STREAMS, 2, L, HEADS * HD), jnp.float32), -6.0, 6.0)
    return drawn.astype(jnp.bfloat16)


def place_ends(array, stream_key, least, top_value):
    longest = array.shape.index(max(array.shape))
    spots = []
    for shift in (0, 1):
        where = [jax.random.randint(jax.random.fold_in(stream_key, axis), (), 0, length) for axis, length in enumerate(array.shape)]
        where[longest] = (where[longest] + shift) % array.shape[longest]
        spots.append(tuple(where))
    return array.at[spots[0]].set(least).at[spots[1]].set(top_value)


def level_of(own_key, shape, shards, least, largest):
    factor_of = 1.0
    for position, shards_of in shards:
        draws = jax.random.uniform(jax.random.fold_in(jax.random.fold_in(own_key, 6), position), (shards_of,), jnp.float32, least / len(shards), largest / len(shards))
        factor_of = factor_of * jnp.repeat(jnp.exp(draws), shape[position] // shards_of).reshape((-1,) + (1,) * (len(shape) - 1 - position))
    return factor_of


def bell_draw(own_key, extent, width, most, split=(), held_as=jnp.bfloat16):
    result = jax.random.normal(own_key, extent, jnp.float32) * width
    if len(split) > 0:
        result = level_of(own_key, extent, split, -0.22, 0.18) * result
    return jnp.clip(result, min=-most, max=most).astype(held_as)


def setup_inputs(seed: int = 0) -> dict:
    keys = jax.random.split(jax.random.key(seed), 8)
    return {
        "residual": bell_draw(keys[0], (STREAMS, D), 1.0, 6.0, ((0, 16), (1, 2))),
        "fresh_qkv": draw_fresh_qkv(jax.random.fold_in(keys[7], 71), 0),
        "active": draw_active(jax.random.fold_in(keys[7], 71), 0),
        "home_slot": draw_home_slot(jax.random.fold_in(keys[7], 71), 0),
        "kv_cache": draw_kv_cache(jax.random.fold_in(keys[7], 71), 0),
        "lengths": place_ends(jax.random.randint(keys[5], (STREAMS,), 2, L + 1), jax.random.fold_in(keys[5], 1), 2, L).astype(jnp.int32),
        "w_out": bell_draw(keys[6], (HEADS * HD, D), (HEADS * HD) ** -0.5, 0.125, ((0, 2),)),
    }


def attend(query, key_rows, value_rows, key_new, value_new, length):
    score_scale = HD ** -0.5
    scores = jnp.einsum("bhd,blhd->bhl", query.astype(jnp.float32), key_rows.astype(jnp.float32)) * score_scale
    positions = jnp.arange(L, dtype=jnp.int32)
    in_cache = positions[None, None, :] < length[:, None, None]
    scores = jnp.where(in_cache, scores, jnp.float32(-1e30))
    own_score = jnp.sum(query.astype(jnp.float32) * key_new.astype(jnp.float32), axis=-1) * score_scale
    row_max = jnp.maximum(jnp.max(scores, axis=-1), own_score)
    weights_raw = jnp.exp(scores - row_max[..., None])
    own_raw = jnp.exp(own_score - row_max)
    denominator = jnp.sum(weights_raw, axis=-1) + own_raw
    weights = (weights_raw / denominator[..., None]).astype(jnp.bfloat16)
    own_weight = (own_raw / denominator).astype(jnp.bfloat16)
    mixed = jnp.einsum("bhl,blhd->bhd", weights.astype(jnp.float32), value_rows.astype(jnp.float32))
    mixed = mixed + own_weight.astype(jnp.float32)[..., None] * value_new.astype(jnp.float32)
    return mixed.astype(jnp.bfloat16).reshape(query.shape[0], -1)


def reference(residual, fresh_qkv, active, home_slot, kv_cache, lengths, w_out):
    groups = STREAMS // S_DEV

    def one_group(group):
        start = (group * S_DEV).astype(jnp.int32)
        streams = start + jnp.arange(S_DEV, dtype=jnp.int32)
        slots = home_slot[streams]
        fresh_rows = jnp.take(fresh_qkv, streams, axis=0).reshape(S_DEV, 3, HEADS, HD)
        cache_rows = jnp.take(kv_cache, slots, axis=0).reshape(S_DEV, 2, L, HEADS, HD)
        attended = attend(fresh_rows[:, 0], cache_rows[:, 0], cache_rows[:, 1], fresh_rows[:, 1], fresh_rows[:, 2], lengths[slots])
        projected = jnp.dot(attended, w_out, preferred_element_type=jnp.float32)
        rows = lax.dynamic_slice_in_dim(residual, start, S_DEV, 0).astype(jnp.float32)
        flags = active[streams].astype(jnp.float32)
        return (rows + flags[:, None] * projected).astype(jnp.bfloat16)

    updated = lax.map(one_group, jnp.arange(groups, dtype=jnp.int32))
    return updated.reshape(STREAMS, D)
```

```python
import functools

import jax
import jax.numpy as jnp
from jax import lax
from jax.experimental import pallas as pl
from jax.experimental.pallas import tpu as pltpu
from jax.sharding import PartitionSpec as P

HD = 128


def attend_local(fresh_rows, kv_cache, lengths, heads_local):
    streams_here = fresh_rows.shape[0]
    cache_len = kv_cache.shape[2]
    head_size = fresh_rows.shape[1] // (3 * heads_local)
    score_scale = head_size ** (-0.5)
    fresh_split = fresh_rows.reshape(streams_here, 3, heads_local, head_size)
    query = fresh_split[:, 0]
    key_rows = kv_cache[:, 0].reshape(streams_here, cache_len, heads_local, head_size)
    value_rows = kv_cache[:, 1].reshape(streams_here, cache_len, heads_local, head_size)
    scores = (
        jnp.einsum("bhd,blhd->bhl", query, key_rows, preferred_element_type=jnp.float32)
        * score_scale
    )
    positions = jnp.arange(cache_len, dtype=jnp.int32)
    in_cache = positions[None, None, :] < lengths[:, None, None]
    scores = jnp.where(in_cache, scores, jnp.float32(-1e30))
    own_score = (
        jnp.sum(query.astype(jnp.float32) * fresh_split[:, 1].astype(jnp.float32), axis=-1)
        * score_scale
    )
    row_max = jnp.maximum(jnp.max(scores, axis=-1), own_score)
    weights_raw = jnp.exp(scores - row_max[..., None])
    own_raw = jnp.exp(own_score - row_max)
    denominator = jnp.sum(weights_raw, axis=-1) + own_raw
    weights = (weights_raw / denominator[..., None]).astype(jnp.bfloat16)
    own_weight = (own_raw / denominator).astype(jnp.bfloat16)
    mixed = jnp.einsum("bhl,blhd->bhd", weights, value_rows, preferred_element_type=jnp.float32)
    mixed = mixed + own_weight.astype(jnp.float32)[..., None] * fresh_split[:, 2].astype(
        jnp.float32
    )
    return mixed.astype(jnp.bfloat16).reshape(streams_here, heads_local * head_size)


def general_body(residual, fresh_qkv, active, home_slot, kv_cache, lengths, w_out):
    groups = lax.axis_size("dp")
    group_here = lax.axis_index("dp")
    streams_here = home_slot.shape[0]
    width_here = fresh_qkv.shape[2]
    heads_local = width_here // HD
    capacity = max(2, streams_here // groups)
    slot_count = groups * capacity
    owner_group = home_slot // streams_here
    is_active = active > 0
    earlier = jnp.arange(streams_here)[:, None] < jnp.arange(streams_here)[None, :]
    same_owner = (
        (owner_group[:, None] == owner_group[None, :])
        & is_active[:, None]
        & is_active[None, :]
        & earlier
    )
    send_rank = jnp.sum(same_owner.astype(jnp.int32), axis=0)
    target = owner_group * capacity + send_rank
    placed = (jnp.arange(slot_count, dtype=jnp.int32)[:, None] == target[None, :]) & is_active[
        None, :
    ]
    placing = placed.astype(jnp.bfloat16)
    fresh_flat = fresh_qkv.reshape(streams_here, 3 * width_here)
    send_rows = jnp.dot(placing, fresh_flat, preferred_element_type=jnp.float32).astype(
        jnp.bfloat16
    )
    send_rows = send_rows.reshape(groups, capacity, 3 * width_here)
    slot_ids = jnp.sum(jnp.where(placed, home_slot[None, :] + 1, 0), axis=1) - 1
    slot_ids = slot_ids.reshape(groups, capacity)
    got_rows, got_ids = (
        lax.all_to_all(send_rows, "dp", split_axis=0, concat_axis=0, tiled=True),
        lax.all_to_all(slot_ids, "dp", split_axis=0, concat_axis=0, tiled=True),
    )
    local_slot = got_ids.reshape(slot_count) - group_here * streams_here
    matched = (local_slot[None, :] == jnp.arange(streams_here, dtype=jnp.int32)[:, None]).astype(
        jnp.bfloat16
    )
    owned = jnp.dot(
        matched, got_rows.reshape(slot_count, 3 * width_here), preferred_element_type=jnp.float32
    ).astype(jnp.bfloat16)
    attended = attend_local(owned, kv_cache, lengths, heads_local)
    heads_rows = jnp.dot(matched.T, attended, preferred_element_type=jnp.float32).astype(
        jnp.bfloat16
    )
    returned = lax.all_to_all(
        heads_rows.reshape(groups, capacity, width_here),
        "dp",
        split_axis=0,
        concat_axis=0,
        tiled=True,
    )
    source_rows = jnp.dot(
        placing.T, returned.reshape(slot_count, width_here), preferred_element_type=jnp.float32
    ).astype(jnp.bfloat16)
    partial_rows = jnp.dot(source_rows, w_out, preferred_element_type=jnp.float32)
    gained = lax.psum_scatter(partial_rows, "tensor", scatter_dimension=1, tiled=True)
    return (residual.astype(jnp.float32) + gained).astype(jnp.bfloat16)


MESH = pl.DeviceIdType.MESH
F32 = jnp.float32
BF16 = jnp.bfloat16
LANES = 128
KV_PARTS = 4
COLUMN_CHUNKS = 4


def partner_of(me, k, n):
    peer = me
    for bit in range(n.bit_length() - 1):
        flip = (k // (1 << bit)) % 2 if isinstance(k, int) else lax.rem(k // (1 << bit), 2)
        peer = peer + flip * (1 - 2 * lax.rem(me // (1 << bit), 2)) * (1 << bit)
    return peer


def iota(shape, dim):
    return lax.broadcasted_iota(jnp.int32, shape, dim)


def kernel(
    n, heads, bounds, home_ref, active_ref, lengths_ref, fresh_hbm, kv_hbm, w_hbm, residual_hbm,
    out_ref,
    fresh, kv, w_mine, w_other, residual, send_q, got_q, send_i, ids, send_a, got_a, send_l, got_l,
    own, value_rows, place_back, attended, part_send, part_got, kept, gained,
    fresh_sem, kv_sem, w_sem, residual_sem, q_send, q_got, i_send, i_got, a_send, a_got, l_send,
    l_got, p_send, p_got,
):
    me = lax.axis_index("dp")
    side = lax.axis_index("tensor")
    other = 1 - side
    streams = home_ref.shape[1]
    width = heads * HD
    capacity = streams // n
    cache_len = kv.shape[2]
    columns = residual.shape[1]
    step = columns // COLUMN_CHUNKS
    scale = HD ** -0.5
    spans = [slice(h * HD, (h + 1) * HD) for h in range(heads)]
    pair = {"tensor": other}

    barrier = pltpu.get_barrier_semaphore()
    for k in range(1, n):
        pl.semaphore_signal(
            barrier, inc=1, device_id={"dp": partner_of(me, k, n)}, device_id_type=MESH
        )
    pl.semaphore_signal(barrier, inc=1, device_id=pair, device_id_type=MESH)

    fresh_copies = [
        pltpu.make_async_copy(fresh_hbm.at[i], fresh.at[i], fresh_sem.at[i]) for i in range(3)
    ]
    fresh_copies[0].start()
    part = streams // KV_PARTS
    kv_copies = [
        pltpu.make_async_copy(
            kv_hbm.at[pl.ds(i * part, part)], kv.at[pl.ds(i * part, part)], kv_sem.at[i]
        )
        for i in range(KV_PARTS)
    ]
    for copy in fresh_copies[1:] + kv_copies:
        copy.start()
    w_copies = [
        pltpu.make_async_copy(
            w_hbm.at[:, pl.ds(pl.multiple_of(at * columns, columns), columns)], dst, w_sem.at[i]
        )
        for i, (at, dst) in enumerate(((other, w_other), (side, w_mine)))
    ]
    for copy in w_copies:
        copy.start()
    residual_copy = pltpu.make_async_copy(residual_hbm, residual, residual_sem)
    residual_copy.start()

    home = home_ref[...]
    is_active = active_ref[...] > 0
    shift = streams.bit_length() - 1
    hop = lax.shift_right_logical(home, shift) ^ me
    local = (home & (streams - 1)).astype(F32)
    square = (streams, streams)
    rows_of = iota((n, streams), 0)
    sent_to = jnp.where((rows_of == hop) & is_active, 1.0, 0.0)
    before = jnp.where(iota(square, 0) < iota(square, 1), 1.0, 0.0).astype(BF16)
    rank = jnp.dot(sent_to.astype(BF16), before, preferred_element_type=F32)
    target = jnp.sum(sent_to * (rank + (rows_of * capacity).astype(F32)), axis=0, keepdims=True)
    target = jnp.where(is_active, target, -1.0)
    placing = jnp.where(iota(square, 0).astype(F32) == target, 1.0, 0.0)
    placed = placing.astype(BF16)
    slot_ids = lax.dot_general(
        jnp.broadcast_to(local, (16, streams)).astype(BF16),
        placed,
        (((1,), (1,)), ((), ())),
        preferred_element_type=F32,
    )
    send_i[...] = slot_ids[:1].astype(jnp.int32)
    fresh_copies[0].wait()
    send_q[...] = (
        jnp.dot(placed, fresh[0], preferred_element_type=F32)
        .astype(BF16)
        .reshape(n, capacity, width)
    )

    def remote(source, landing, send_sem, got_sem, k):
        return pltpu.make_async_remote_copy(
            src_ref=source,
            dst_ref=landing,
            send_sem=send_sem.at[k],
            recv_sem=got_sem.at[k],
            device_id={"dp": partner_of(me, k, n)},
            device_id_type=MESH,
        )

    def query_copy(k):
        return remote(send_q.at[k], got_q.at[k], q_send, q_got, k)

    def id_copy(k):
        return remote(send_i, ids.at[k], i_send, i_got, k)

    def back_copy(k):
        return remote(send_a.at[k], got_a.at[k], a_send, a_got, k)

    def lse_copy(k):
        return remote(send_l.at[k], got_l.at[k], l_send, l_got, k)

    query_here = pltpu.make_async_copy(send_q.at[0], got_q.at[0], q_got.at[0])
    ids_here = pltpu.make_async_copy(send_i, ids.at[0], i_got.at[0])
    back_here = pltpu.make_async_copy(send_a.at[0], got_a.at[0], a_got.at[0])
    lse_here = pltpu.make_async_copy(send_l.at[0], got_l.at[0], l_got.at[0])

    ids_here.start()
    query_here.start()
    pl.semaphore_wait(barrier, n)
    for k in range(1, n):
        id_copy(k).start()
        query_copy(k).start()

    for copy in fresh_copies[1:]:
        copy.wait()
    key_rows = jnp.dot(placed, fresh[1], preferred_element_type=F32).astype(BF16)
    value_rows[...] = jnp.dot(placed, fresh[2], preferred_element_type=F32).astype(BF16)
    lane = iota((streams, LANES), 1)
    own_scores = jnp.zeros((streams, LANES), F32)
    for h, span in enumerate(spans):
        query = send_q[:, :, span].reshape(streams, HD).astype(F32)
        key = key_rows[:, span].astype(F32)
        own_h = jnp.sum(query * key, axis=1, keepdims=True) * scale
        own_scores = jnp.where(lane == h, own_h, own_scores)
    own[...] = own_scores
    turned = jnp.transpose(placing).astype(BF16)
    place_back[...] = jnp.concatenate([turned, turned], axis=1)
    for copy in kv_copies:
        copy.wait()

    reach = (capacity, capacity * cache_len)
    offset = iota(reach, 1) - iota(reach, 0) * cache_len
    row_index = iota(reach, 0)
    eye = iota((LANES, LANES), 0) == iota((LANES, LANES), 1)

    def attend(k, carry):
        @pl.when(k == 0)
        def _():
            ids_here.wait()
            query_here.wait()

        @pl.when(k > 0)
        def _():
            id_copy(k).wait_recv()
            query_copy(k).wait_recv()

        slots = [
            jnp.clip(ids[k, 0, k * capacity + i], 0, streams - 1) for i in range(capacity)
        ]
        limit = jnp.zeros(reach, jnp.int32)
        for i, slot in enumerate(slots):
            limit = jnp.where(row_index == i, lengths_ref[0, slot], limit)
        valid = (offset >= 0) & (offset < limit)
        valid = jnp.concatenate([jnp.where(valid, 1.0, 0.0)] * heads, axis=0) > 0
        scores = jnp.concatenate(
            [
                lax.dot_general(
                    got_q[k, :, span],
                    jnp.concatenate([kv[slot, 0, :, span] for slot in slots], axis=0),
                    (((1,), (1,)), ((), ())),
                    preferred_element_type=F32,
                )
                for span in spans
            ],
            axis=0,
        )
        scores = jnp.where(valid, scores * scale, -1e30)
        top = jnp.max(scores, axis=1, keepdims=True)
        raw = jnp.exp(scores - top)
        total = jnp.sum(raw, axis=1, keepdims=True)
        weights = (raw / total).astype(BF16)
        lse = top + jnp.log(total)
        send_l[k] = jnp.sum(jnp.where(eye, lse, 0.0), axis=0, keepdims=True)
        for h, span in enumerate(spans):
            send_a[k, :, span] = jnp.dot(
                weights[h * capacity : (h + 1) * capacity],
                jnp.concatenate([kv[slot, 1, :, span] for slot in slots], axis=0),
                preferred_element_type=F32,
            ).astype(BF16)

        @pl.when(k == 0)
        def _():
            lse_here.start()
            back_here.start()

        @pl.when(k > 0)
        def _():
            lse_copy(k).start()
            back_copy(k).start()

        return carry

    def part_copy(g, c):
        rows = pl.ds(bounds[g] * capacity, (bounds[g + 1] - bounds[g]) * capacity)
        return pltpu.make_async_remote_copy(
            src_ref=part_send.at[c, rows],
            dst_ref=part_got.at[c, rows],
            send_sem=p_send.at[g, c],
            recv_sem=p_got.at[g, c],
            device_id=pair,
            device_id_type=MESH,
        )

    def project(g):
        first, last = bounds[g], bounds[g + 1]
        rows = slice(first * capacity, last * capacity)
        count = (last - first) * capacity
        for k in range(first, last):
            if k:
                back_copy(k).wait_recv()
                lse_copy(k).wait_recv()
            else:
                back_here.wait()
                lse_here.wait()
        arrived = got_a[first:last].reshape(count, width)
        own_rows = own[rows]
        turned = [
            jnp.sum(jnp.where(eye, got_l[k], 0.0), axis=1, keepdims=True)
            for k in range(first, last)
        ]
        for h, span in enumerate(spans):
            lse = jnp.concatenate(
                [column[h * capacity : (h + 1) * capacity] for column in turned], axis=0
            )
            own_h = own_rows[:, h : h + 1]
            top = jnp.maximum(lse, own_h)
            from_cache = jnp.exp(lse - top)
            from_own = jnp.exp(own_h - top)
            share = 1.0 / (from_cache + from_own)
            attended[rows, span] = (
                (from_cache * share) * arrived[:, span].astype(F32)
                + (from_own * share) * value_rows[rows, span].astype(F32)
            ).astype(BF16)
        if g == 0:
            for copy in w_copies:
                copy.wait()
        for c in range(COLUMN_CHUNKS):
            here = slice(c * step, (c + 1) * step)
            part_send[c, rows] = jnp.dot(
                attended[rows], w_other[:, here], preferred_element_type=F32
            ).astype(BF16)
            part_copy(g, c).start()
        for c in range(COLUMN_CHUNKS):
            here = slice(c * step, (c + 1) * step)
            kept[c, rows] = jnp.dot(attended[rows], w_mine[:, here], preferred_element_type=F32)

    def gather(g, c):
        first, last = bounds[g] * capacity, bounds[g + 1] * capacity
        part_copy(g, c).wait()
        total = kept[c, first:last] + part_got[c, first:last].astype(F32)
        high = total.astype(BF16)
        gained[c, first:last] = high
        gained[c, streams + first : streams + last] = (total - high.astype(F32)).astype(BF16)

    groups = len(bounds) - 1
    for g in range(groups):
        lax.fori_loop(bounds[g], bounds[g + 1], attend, 0)
        if g:
            project(g - 1)
    project(groups - 1)
    residual_copy.wait()
    for g in range(groups - 1):
        for c in range(COLUMN_CHUNKS):
            gather(g, c)
    for c in range(COLUMN_CHUNKS):
        gather(groups - 1, c)
        span = slice(c * step, (c + 1) * step)
        out_ref[:, span] = (
            residual[:, span].astype(F32)
            + jnp.dot(place_back[...], gained[c], preferred_element_type=F32)
        ).astype(BF16)
    for k in range(1, n):
        id_copy(k).wait_send()
        query_copy(k).wait_send()
        back_copy(k).wait_send()
        lse_copy(k).wait_send()


def fused_body(residual, fresh_qkv, active, home_slot, kv_cache, lengths, w_out):
    n = lax.axis_size("dp")
    streams, columns = residual.shape
    width = fresh_qkv.shape[2]
    heads = width // HD
    capacity = streams // n
    quarter = n // 4
    bounds = (0, quarter, 2 * quarter, 3 * quarter, 3 * quarter + quarter // 2, n)
    groups = len(bounds) - 1
    rows = (n, capacity, width)
    lse_rows = (n, 1, heads * capacity)
    step = columns // COLUMN_CHUNKS
    vmem = pl.BlockSpec(memory_space=pltpu.VMEM)
    smem = pl.BlockSpec(memory_space=pltpu.SMEM)
    anywhere = pl.BlockSpec(memory_space=pl.ANY)
    dma = pltpu.SemaphoreType.DMA
    return pl.pallas_call(
        functools.partial(kernel, n, heads, bounds),
        out_shape=pltpu.VMEM((streams, columns), BF16),
        in_specs=[vmem] * 2 + [smem] + [anywhere] * 4,
        out_specs=vmem,
        scratch_shapes=[
            pltpu.VMEM((3, streams, width), BF16),
            pltpu.VMEM(kv_cache.shape, BF16),
            pltpu.VMEM((w_out.shape[0], columns), BF16),
            pltpu.VMEM((w_out.shape[0], columns), BF16),
            pltpu.VMEM(residual.shape, BF16),
            pltpu.VMEM(rows, BF16),
            pltpu.VMEM(rows, BF16),
            pltpu.VMEM((1, streams), jnp.int32),
            pltpu.SMEM((n, 1, streams), jnp.int32),
            pltpu.VMEM(rows, BF16),
            pltpu.VMEM(rows, BF16),
            pltpu.VMEM(lse_rows, F32),
            pltpu.VMEM(lse_rows, F32),
            pltpu.VMEM((streams, LANES), F32),
            pltpu.VMEM((streams, width), BF16),
            pltpu.VMEM((streams, 2 * streams), BF16),
            pltpu.VMEM((streams, width), BF16),
            pltpu.VMEM((COLUMN_CHUNKS, streams, step), BF16),
            pltpu.VMEM((COLUMN_CHUNKS, streams, step), BF16),
            pltpu.VMEM((COLUMN_CHUNKS, streams, step), F32),
            pltpu.VMEM((COLUMN_CHUNKS, 2 * streams, step), BF16),
            dma((3,)),
            dma((KV_PARTS,)),
            dma((2,)),
            dma,
        ]
        + [dma((n,))] * 8
        + [dma((groups, COLUMN_CHUNKS))] * 2,
        compiler_params=pltpu.CompilerParams(
            collective_id=0, has_side_effects=True, vmem_limit_bytes=60 * 1024 * 1024
        ),
    )(
        home_slot.reshape(1, streams),
        active.reshape(1, streams),
        lengths.reshape(1, streams),
        jnp.transpose(fresh_qkv, (1, 0, 2)),
        kv_cache,
        w_out,
        residual,
    )


def body(residual, fresh_qkv, active, home_slot, kv_cache, lengths, w_out):
    n = lax.axis_size("dp")
    streams = home_slot.shape[0]
    heads = fresh_qkv.shape[2] // HD
    fits = (
        lax.axis_size("tensor") == 2
        and n % 8 == 0
        and n & (n - 1) == 0
        and streams == 16 * n
        and streams <= 256
        and heads * 16 == LANES
        and kv_cache.shape[2] == 16
    )
    chosen = fused_body if fits else general_body
    return chosen(residual, fresh_qkv, active, home_slot, kv_cache, lengths, w_out)


def solution(mesh):
    placed = (
        P("dp", "tensor"),
        P("dp", None, "tensor"),
        P("dp"),
        P("dp"),
        P("dp", None, None, "tensor"),
        P("dp"),
        P("tensor", None),
    )
    return jax.shard_map(
        body, mesh=mesh, in_specs=placed, out_specs=P("dp", "tensor"), check_vma=False
    )
```

```python
import functools

import jax
import jax.numpy as jnp
from jax import lax
from jax.experimental import pallas as pl
from jax.experimental.pallas import tpu as pltpu
from jax.sharding import PartitionSpec as P

HD = 128


def attend_local(fresh_rows, kv_cache, lengths, heads_local):
    streams_here = fresh_rows.shape[0]
    cache_len = kv_cache.shape[2]
    head_size = fresh_rows.shape[1] // (3 * heads_local)
    score_scale = head_size ** (-0.5)
    fresh_split = fresh_rows.reshape(streams_here, 3, heads_local, head_size)
    query = fresh_split[:, 0]
    key_rows = kv_cache[:, 0].reshape(streams_here, cache_len, heads_local, head_size)
    value_rows = kv_cache[:, 1].reshape(streams_here, cache_len, heads_local, head_size)
    scores = (
        jnp.einsum("bhd,blhd->bhl", query, key_rows, preferred_element_type=jnp.float32)
        * score_scale
    )
    positions = jnp.arange(cache_len, dtype=jnp.int32)
    in_cache = positions[None, None, :] < lengths[:, None, None]
    scores = jnp.where(in_cache, scores, jnp.float32(-1e30))
    own_score = (
        jnp.sum(query.astype(jnp.float32) * fresh_split[:, 1].astype(jnp.float32), axis=-1)
        * score_scale
    )
    row_max = jnp.maximum(jnp.max(scores, axis=-1), own_score)
    weights_raw = jnp.exp(scores - row_max[..., None])
    own_raw = jnp.exp(own_score - row_max)
    denominator = jnp.sum(weights_raw, axis=-1) + own_raw
    weights = (weights_raw / denominator[..., None]).astype(jnp.bfloat16)
    own_weight = (own_raw / denominator).astype(jnp.bfloat16)
    mixed = jnp.einsum("bhl,blhd->bhd", weights, value_rows, preferred_element_type=jnp.float32)
    mixed = mixed + own_weight.astype(jnp.float32)[..., None] * fresh_split[:, 2].astype(
        jnp.float32
    )
    return mixed.astype(jnp.bfloat16).reshape(streams_here, heads_local * head_size)


def general_body(residual, fresh_qkv, active, home_slot, kv_cache, lengths, w_out):
    groups = lax.axis_size("dp")
    group_here = lax.axis_index("dp")
    streams_here = home_slot.shape[0]
    width_here = fresh_qkv.shape[2]
    heads_local = width_here // HD
    capacity = max(2, streams_here // groups)
    slot_count = groups * capacity
    owner_group = home_slot // streams_here
    is_active = active > 0
    earlier = jnp.arange(streams_here)[:, None] < jnp.arange(streams_here)[None, :]
    same_owner = (
        (owner_group[:, None] == owner_group[None, :])
        & is_active[:, None]
        & is_active[None, :]
        & earlier
    )
    send_rank = jnp.sum(same_owner.astype(jnp.int32), axis=0)
    target = owner_group * capacity + send_rank
    placed = (jnp.arange(slot_count, dtype=jnp.int32)[:, None] == target[None, :]) & is_active[
        None, :
    ]
    placing = placed.astype(jnp.bfloat16)
    fresh_flat = fresh_qkv.reshape(streams_here, 3 * width_here)
    send_rows = jnp.dot(placing, fresh_flat, preferred_element_type=jnp.float32).astype(
        jnp.bfloat16
    )
    send_rows = send_rows.reshape(groups, capacity, 3 * width_here)
    slot_ids = jnp.sum(jnp.where(placed, home_slot[None, :] + 1, 0), axis=1) - 1
    slot_ids = slot_ids.reshape(groups, capacity)
    got_rows, got_ids = (
        lax.all_to_all(send_rows, "dp", split_axis=0, concat_axis=0, tiled=True),
        lax.all_to_all(slot_ids, "dp", split_axis=0, concat_axis=0, tiled=True),
    )
    local_slot = got_ids.reshape(slot_count) - group_here * streams_here
    matched = (local_slot[None, :] == jnp.arange(streams_here, dtype=jnp.int32)[:, None]).astype(
        jnp.bfloat16
    )
    owned = jnp.dot(
        matched, got_rows.reshape(slot_count, 3 * width_here), preferred_element_type=jnp.float32
    ).astype(jnp.bfloat16)
    attended = attend_local(owned, kv_cache, lengths, heads_local)
    heads_rows = jnp.dot(matched.T, attended, preferred_element_type=jnp.float32).astype(
        jnp.bfloat16
    )
    returned = lax.all_to_all(
        heads_rows.reshape(groups, capacity, width_here),
        "dp",
        split_axis=0,
        concat_axis=0,
        tiled=True,
    )
    source_rows = jnp.dot(
        placing.T, returned.reshape(slot_count, width_here), preferred_element_type=jnp.float32
    ).astype(jnp.bfloat16)
    partial_rows = jnp.dot(source_rows, w_out, preferred_element_type=jnp.float32)
    gained = lax.psum_scatter(partial_rows, "tensor", scatter_dimension=1, tiled=True)
    return (residual.astype(jnp.float32) + gained).astype(jnp.bfloat16)


MESH = pl.DeviceIdType.MESH
F32 = jnp.float32
BF16 = jnp.bfloat16
LANES = 128
KV_PARTS = 4
COLUMN_CHUNKS = 2


def partner_of(me, k, n):
    peer = me
    for bit in range(n.bit_length() - 1):
        flip = (k // (1 << bit)) % 2 if isinstance(k, int) else lax.rem(k // (1 << bit), 2)
        peer = peer + flip * (1 - 2 * lax.rem(me // (1 << bit), 2)) * (1 << bit)
    return peer


def iota(shape, dim):
    return lax.broadcasted_iota(jnp.int32, shape, dim)


def kernel(
    n, heads, plan, home_ref, active_ref, lengths_ref, fresh_hbm, kv_hbm, w_hbm, residual_hbm,
    out_ref,
    fresh, kv, w_mine, w_other, residual, send_q, got_q, send_i, ids, send_a, got_a, send_l, got_l,
    own, value_rows, place_back, attended, part_send, part_got, kept, gained,
    fresh_sem, kv_sem, w_sem, residual_sem, q_send, q_got, i_send, i_got, a_send, a_got, l_send,
    l_got, p_send, p_got,
):
    me = lax.axis_index("dp")
    side = lax.axis_index("tensor")
    other = 1 - side
    streams = home_ref.shape[1]
    width = heads * HD
    capacity = streams // n
    cache_len = kv.shape[2]
    columns = residual.shape[1]
    step = columns // COLUMN_CHUNKS
    scale = HD ** -0.5
    spans = [slice(h * HD, (h + 1) * HD) for h in range(heads)]
    pair = {"tensor": other}

    barrier = pltpu.get_barrier_semaphore()
    for k in range(1, n):
        pl.semaphore_signal(
            barrier, inc=1, device_id={"dp": partner_of(me, k, n)}, device_id_type=MESH
        )
    pl.semaphore_signal(barrier, inc=1, device_id=pair, device_id_type=MESH)

    fresh_copies = [
        pltpu.make_async_copy(fresh_hbm.at[i], fresh.at[i], fresh_sem.at[i]) for i in range(3)
    ]
    fresh_copies[0].start()
    part = streams // KV_PARTS
    kv_copies = [
        pltpu.make_async_copy(
            kv_hbm.at[pl.ds(i * part, part)], kv.at[pl.ds(i * part, part)], kv_sem.at[i]
        )
        for i in range(KV_PARTS)
    ]
    for copy in fresh_copies[1:] + kv_copies:
        copy.start()
    w_copies = [
        pltpu.make_async_copy(
            w_hbm.at[:, pl.ds(pl.multiple_of(at * columns, columns), columns)], dst, w_sem.at[i]
        )
        for i, (at, dst) in enumerate(((other, w_other), (side, w_mine)))
    ]
    residual_copy = pltpu.make_async_copy(residual_hbm, residual, residual_sem)

    home = home_ref[...]
    is_active = active_ref[...] > 0
    shift = streams.bit_length() - 1
    hop = lax.shift_right_logical(home, shift) ^ me
    local = (home & (streams - 1)).astype(F32)
    square = (streams, streams)
    rows_of = iota((n, streams), 0)
    sent_to = jnp.where((rows_of == hop) & is_active, 1.0, 0.0)
    before = jnp.where(iota(square, 0) < iota(square, 1), 1.0, 0.0).astype(BF16)
    rank = jnp.dot(sent_to.astype(BF16), before, preferred_element_type=F32)
    target = jnp.sum(sent_to * (rank + (rows_of * capacity).astype(F32)), axis=0, keepdims=True)
    target = jnp.where(is_active, target, -1.0)
    placing = jnp.where(iota(square, 0).astype(F32) == target, 1.0, 0.0)
    placed = placing.astype(BF16)
    slot_ids = lax.dot_general(
        jnp.broadcast_to(local, (16, streams)).astype(BF16),
        placed,
        (((1,), (1,)), ((), ())),
        preferred_element_type=F32,
    )
    send_i[...] = slot_ids[:1].astype(jnp.int32)
    fresh_copies[0].wait()
    for copy in w_copies:
        copy.start()
    residual_copy.start()
    send_q[...] = (
        jnp.dot(placed, fresh[0], preferred_element_type=F32)
        .astype(BF16)
        .reshape(n, capacity, width)
    )

    def remote(source, landing, send_sem, got_sem, k):
        return pltpu.make_async_remote_copy(
            src_ref=source,
            dst_ref=landing,
            send_sem=send_sem.at[k],
            recv_sem=got_sem.at[k],
            device_id={"dp": partner_of(me, k, n)},
            device_id_type=MESH,
        )

    def query_copy(k):
        return remote(send_q.at[k], got_q.at[k], q_send, q_got, k)

    def id_copy(k):
        return remote(send_i, ids.at[k], i_send, i_got, k)

    def back_copy(k):
        return remote(send_a.at[k], got_a.at[k], a_send, a_got, k)

    def lse_copy(k):
        return remote(send_l.at[k], got_l.at[k], l_send, l_got, k)

    query_here = pltpu.make_async_copy(send_q.at[0], got_q.at[0], q_got.at[0])
    ids_here = pltpu.make_async_copy(send_i, ids.at[0], i_got.at[0])
    back_here = pltpu.make_async_copy(send_a.at[0], got_a.at[0], a_got.at[0])
    lse_here = pltpu.make_async_copy(send_l.at[0], got_l.at[0], l_got.at[0])

    ids_here.start()
    query_here.start()
    pl.semaphore_wait(barrier, n)
    for k in range(1, n):
        id_copy(k).start()
        query_copy(k).start()

    for copy in fresh_copies[1:]:
        copy.wait()
    key_rows = jnp.dot(placed, fresh[1], preferred_element_type=F32).astype(BF16)
    value_rows[...] = jnp.dot(placed, fresh[2], preferred_element_type=F32).astype(BF16)
    lane = iota((streams, LANES), 1)
    own_scores = jnp.zeros((streams, LANES), F32)
    for h, span in enumerate(spans):
        query = send_q[:, :, span].reshape(streams, HD).astype(F32)
        key = key_rows[:, span].astype(F32)
        own_h = jnp.sum(query * key, axis=1, keepdims=True) * scale
        own_scores = jnp.where(lane == h, own_h, own_scores)
    own[...] = own_scores
    for copy in kv_copies:
        copy.wait()

    reach = (capacity, capacity * cache_len)
    offset = iota(reach, 1) - iota(reach, 0) * cache_len
    row_index = iota(reach, 0)
    eye = iota((LANES, LANES), 0) == iota((LANES, LANES), 1)

    def attend(k, carry):
        @pl.when(k == 0)
        def _():
            ids_here.wait()
            query_here.wait()

        @pl.when(k > 0)
        def _():
            id_copy(k).wait_recv()
            query_copy(k).wait_recv()

        slots = [
            jnp.clip(ids[k, 0, k * capacity + i], 0, streams - 1) for i in range(capacity)
        ]
        limit = jnp.zeros(reach, jnp.int32)
        for i, slot in enumerate(slots):
            limit = jnp.where(row_index == i, lengths_ref[0, slot], limit)
        valid = (offset >= 0) & (offset < limit)
        valid = jnp.concatenate([jnp.where(valid, 1.0, 0.0)] * heads, axis=0) > 0
        scores = jnp.concatenate(
            [
                lax.dot_general(
                    got_q[k, :, span],
                    jnp.concatenate([kv[slot, 0, :, span] for slot in slots], axis=0),
                    (((1,), (1,)), ((), ())),
                    preferred_element_type=F32,
                )
                for span in spans
            ],
            axis=0,
        )
        scores = jnp.where(valid, scores * scale, -1e30)
        top = jnp.max(scores, axis=1, keepdims=True)
        raw = jnp.exp(scores - top)
        total = jnp.sum(raw, axis=1, keepdims=True)
        weights = (raw / total).astype(BF16)
        lse = top + jnp.log(total)
        send_l[k] = jnp.sum(jnp.where(eye, lse, 0.0), axis=0, keepdims=True)
        for h, span in enumerate(spans):
            send_a[k, :, span] = jnp.dot(
                weights[h * capacity : (h + 1) * capacity],
                jnp.concatenate([kv[slot, 1, :, span] for slot in slots], axis=0),
                preferred_element_type=F32,
            ).astype(BF16)

        @pl.when(k == 0)
        def _():
            lse_here.start()
            back_here.start()

        @pl.when(k > 0)
        def _():
            lse_copy(k).start()
            back_copy(k).start()

        return carry

    def part_copy(first, last, c):
        rows = pl.ds(first * capacity, (last - first) * capacity)
        return pltpu.make_async_remote_copy(
            src_ref=part_send.at[c, rows],
            dst_ref=part_got.at[c, rows],
            send_sem=p_send.at[first, c],
            recv_sem=p_got.at[first, c],
            device_id=pair,
            device_id_type=MESH,
        )

    def project(first, last):
        rows = slice(first * capacity, last * capacity)
        for k in range(first, last):
            if k:
                back_copy(k).wait_recv()
                lse_copy(k).wait_recv()
            else:
                back_here.wait()
                lse_here.wait()
        arrived = got_a[first:last].reshape((last - first) * capacity, width)
        own_rows = own[rows]
        turned = [
            jnp.sum(jnp.where(eye, got_l[k], 0.0), axis=1, keepdims=True)
            for k in range(first, last)
        ]
        for h, span in enumerate(spans):
            lse = jnp.concatenate(
                [column[h * capacity : (h + 1) * capacity] for column in turned], axis=0
            )
            own_h = own_rows[:, h : h + 1]
            top = jnp.maximum(lse, own_h)
            from_cache = jnp.exp(lse - top)
            from_own = jnp.exp(own_h - top)
            share = 1.0 / (from_cache + from_own)
            attended[rows, span] = (
                (from_cache * share) * arrived[:, span].astype(F32)
                + (from_own * share) * value_rows[rows, span].astype(F32)
            ).astype(BF16)
        if first == 0:
            w_copies[0].wait()
        for c in range(COLUMN_CHUNKS):
            part_send[c, rows] = jnp.dot(
                attended[rows], w_other[:, c * step : (c + 1) * step], preferred_element_type=F32
            ).astype(BF16)
            part_copy(first, last, c).start()

    def keep(first, last):
        rows = slice(first * capacity, last * capacity)
        if first == 0:
            w_copies[1].wait()
        for c in range(COLUMN_CHUNKS):
            kept[c, rows] = jnp.dot(
                attended[rows], w_mine[:, c * step : (c + 1) * step], preferred_element_type=F32
            )

    def gather(first, last, c):
        rows = slice(first * capacity, last * capacity)
        for begin, end in sends:
            if first <= begin < last:
                part_copy(begin, end, c).wait()
        total = kept[c, rows] + part_got[c, rows].astype(F32)
        high = total.astype(BF16)
        gained[c, rows] = high
        gained[c, streams + first * capacity : streams + last * capacity] = (
            total - high.astype(F32)
        ).astype(BF16)

    sends = [(first, last) for what, first, last in plan if what == "project"]
    for what, first, last in plan:
        if what == "attend":
            lax.fori_loop(first, last, attend, 0)
        elif what == "project":
            project(first, last)
        else:
            keep(first, last)
    turned = jnp.transpose(placing).astype(BF16)
    place_back[...] = jnp.concatenate([turned, turned], axis=1)
    residual_copy.wait()
    late = n - n // 4
    for c in range(COLUMN_CHUNKS):
        gather(0, late, c)
    for c in range(COLUMN_CHUNKS):
        gather(late, n, c)
        span = slice(c * step, (c + 1) * step)
        out_ref[:, span] = (
            residual[:, span].astype(F32)
            + jnp.dot(place_back[...], gained[c], preferred_element_type=F32)
        ).astype(BF16)
    for k in range(1, n):
        id_copy(k).wait_send()
        query_copy(k).wait_send()
        back_copy(k).wait_send()
        lse_copy(k).wait_send()


def steps_of(n):
    q = n // 4
    return (
        ("attend", 0, 1),
        ("project", 0, 1),
        ("attend", 1, q),
        ("project", 1, 2),
        ("project", 2, q),
        ("attend", q, 2 * q),
        ("keep", 0, q),
        ("attend", 2 * q, 3 * q),
        ("project", q, q + 2),
        ("attend", 3 * q, 3 * q + 1),
        ("project", q + 2, 2 * q),
        ("attend", 3 * q + 1, 3 * q + 2),
        ("project", 2 * q, 2 * q + 2),
        ("attend", 3 * q + 2, n),
        ("project", 2 * q + 2, 3 * q),
        ("keep", q, 2 * q),
        ("project", 3 * q, 3 * q + 2),
        ("project", 3 * q + 2, n - 1),
        ("project", n - 1, n),
        ("keep", 2 * q, 3 * q),
        ("keep", 3 * q, n),
    )


def fused_body(residual, fresh_qkv, active, home_slot, kv_cache, lengths, w_out):
    n = lax.axis_size("dp")
    streams, columns = residual.shape
    width = fresh_qkv.shape[2]
    heads = width // HD
    capacity = streams // n
    plan = steps_of(n)
    rows = (n, capacity, width)
    lse_rows = (n, 1, heads * capacity)
    step = columns // COLUMN_CHUNKS
    vmem = pl.BlockSpec(memory_space=pltpu.VMEM)
    smem = pl.BlockSpec(memory_space=pltpu.SMEM)
    anywhere = pl.BlockSpec(memory_space=pl.ANY)
    dma = pltpu.SemaphoreType.DMA
    return pl.pallas_call(
        functools.partial(kernel, n, heads, plan),
        out_shape=pltpu.VMEM((streams, columns), BF16),
        in_specs=[vmem] * 2 + [smem] + [anywhere] * 4,
        out_specs=vmem,
        scratch_shapes=[
            pltpu.VMEM((3, streams, width), BF16),
            pltpu.VMEM(kv_cache.shape, BF16),
            pltpu.VMEM((w_out.shape[0], columns), BF16),
            pltpu.VMEM((w_out.shape[0], columns), BF16),
            pltpu.VMEM(residual.shape, BF16),
            pltpu.VMEM(rows, BF16),
            pltpu.VMEM(rows, BF16),
            pltpu.VMEM((1, streams), jnp.int32),
            pltpu.SMEM((n, 1, streams), jnp.int32),
            pltpu.VMEM(rows, BF16),
            pltpu.VMEM(rows, BF16),
            pltpu.VMEM(lse_rows, F32),
            pltpu.VMEM(lse_rows, F32),
            pltpu.VMEM((streams, LANES), F32),
            pltpu.VMEM((streams, width), BF16),
            pltpu.VMEM((streams, 2 * streams), BF16),
            pltpu.VMEM((streams, width), BF16),
            pltpu.VMEM((COLUMN_CHUNKS, streams, step), BF16),
            pltpu.VMEM((COLUMN_CHUNKS, streams, step), BF16),
            pltpu.VMEM((COLUMN_CHUNKS, streams, step), F32),
            pltpu.VMEM((COLUMN_CHUNKS, 2 * streams, step), BF16),
            dma((3,)),
            dma((KV_PARTS,)),
            dma((2,)),
            dma,
        ]
        + [dma((n,))] * 8
        + [dma((n, COLUMN_CHUNKS))] * 2,
        compiler_params=pltpu.CompilerParams(
            collective_id=0, has_side_effects=True, vmem_limit_bytes=60 * 1024 * 1024
        ),
    )(
        home_slot.reshape(1, streams),
        active.reshape(1, streams),
        lengths.reshape(1, streams),
        jnp.transpose(fresh_qkv, (1, 0, 2)),
        kv_cache,
        w_out,
        residual,
    )


def body(residual, fresh_qkv, active, home_slot, kv_cache, lengths, w_out):
    n = lax.axis_size("dp")
    streams = home_slot.shape[0]
    heads = fresh_qkv.shape[2] // HD
    fits = (
        lax.axis_size("tensor") == 2
        and n % 16 == 0
        and n & (n - 1) == 0
        and streams == 16 * n
        and streams <= 256
        and heads * 16 == LANES
        and kv_cache.shape[2] == 16
    )
    chosen = fused_body if fits else general_body
    return chosen(residual, fresh_qkv, active, home_slot, kv_cache, lengths, w_out)


def solution(mesh):
    placed = (
        P("dp", "tensor"),
        P("dp", None, "tensor"),
        P("dp"),
        P("dp"),
        P("dp", None, None, "tensor"),
        P("dp"),
        P("tensor", None),
    )
    return jax.shard_map(
        body, mesh=mesh, in_specs=placed, out_specs=P("dp", "tensor"), check_vma=False
    )
```

```python
import functools

import jax
import jax.numpy as jnp
from jax import lax
from jax.experimental import pallas as pl
from jax.experimental.pallas import tpu as pltpu
from jax.sharding import PartitionSpec as P

HD = 128


def attend_local(fresh_rows, kv_cache, lengths, heads_local):
    streams_here = fresh_rows.shape[0]
    cache_len = kv_cache.shape[2]
    head_size = fresh_rows.shape[1] // (3 * heads_local)
    score_scale = head_size ** (-0.5)
    fresh_split = fresh_rows.reshape(streams_here, 3, heads_local, head_size)
    query = fresh_split[:, 0]
    key_rows = kv_cache[:, 0].reshape(streams_here, cache_len, heads_local, head_size)
    value_rows = kv_cache[:, 1].reshape(streams_here, cache_len, heads_local, head_size)
    scores = (
        jnp.einsum("bhd,blhd->bhl", query, key_rows, preferred_element_type=jnp.float32)
        * score_scale
    )
    positions = jnp.arange(cache_len, dtype=jnp.int32)
    in_cache = positions[None, None, :] < lengths[:, None, None]
    scores = jnp.where(in_cache, scores, jnp.float32(-1e30))
    own_score = (
        jnp.sum(query.astype(jnp.float32) * fresh_split[:, 1].astype(jnp.float32), axis=-1)
        * score_scale
    )
    row_max = jnp.maximum(jnp.max(scores, axis=-1), own_score)
    weights_raw = jnp.exp(scores - row_max[..., None])
    own_raw = jnp.exp(own_score - row_max)
    denominator = jnp.sum(weights_raw, axis=-1) + own_raw
    weights = (weights_raw / denominator[..., None]).astype(jnp.bfloat16)
    own_weight = (own_raw / denominator).astype(jnp.bfloat16)
    mixed = jnp.einsum("bhl,blhd->bhd", weights, value_rows, preferred_element_type=jnp.float32)
    mixed = mixed + own_weight.astype(jnp.float32)[..., None] * fresh_split[:, 2].astype(
        jnp.float32
    )
    return mixed.astype(jnp.bfloat16).reshape(streams_here, heads_local * head_size)


def general_body(residual, fresh_qkv, active, home_slot, kv_cache, lengths, w_out):
    groups = lax.axis_size("dp")
    group_here = lax.axis_index("dp")
    streams_here = home_slot.shape[0]
    width_here = fresh_qkv.shape[2]
    heads_local = width_here // HD
    capacity = max(2, streams_here // groups)
    slot_count = groups * capacity
    owner_group = home_slot // streams_here
    is_active = active > 0
    earlier = jnp.arange(streams_here)[:, None] < jnp.arange(streams_here)[None, :]
    same_owner = (
        (owner_group[:, None] == owner_group[None, :])
        & is_active[:, None]
        & is_active[None, :]
        & earlier
    )
    send_rank = jnp.sum(same_owner.astype(jnp.int32), axis=0)
    target = owner_group * capacity + send_rank
    placed = (jnp.arange(slot_count, dtype=jnp.int32)[:, None] == target[None, :]) & is_active[
        None, :
    ]
    placing = placed.astype(jnp.bfloat16)
    fresh_flat = fresh_qkv.reshape(streams_here, 3 * width_here)
    send_rows = jnp.dot(placing, fresh_flat, preferred_element_type=jnp.float32).astype(
        jnp.bfloat16
    )
    send_rows = send_rows.reshape(groups, capacity, 3 * width_here)
    slot_ids = jnp.sum(jnp.where(placed, home_slot[None, :] + 1, 0), axis=1) - 1
    slot_ids = slot_ids.reshape(groups, capacity)
    got_rows, got_ids = (
        lax.all_to_all(send_rows, "dp", split_axis=0, concat_axis=0, tiled=True),
        lax.all_to_all(slot_ids, "dp", split_axis=0, concat_axis=0, tiled=True),
    )
    local_slot = got_ids.reshape(slot_count) - group_here * streams_here
    matched = (local_slot[None, :] == jnp.arange(streams_here, dtype=jnp.int32)[:, None]).astype(
        jnp.bfloat16
    )
    owned = jnp.dot(
        matched, got_rows.reshape(slot_count, 3 * width_here), preferred_element_type=jnp.float32
    ).astype(jnp.bfloat16)
    attended = attend_local(owned, kv_cache, lengths, heads_local)
    heads_rows = jnp.dot(matched.T, attended, preferred_element_type=jnp.float32).astype(
        jnp.bfloat16
    )
    returned = lax.all_to_all(
        heads_rows.reshape(groups, capacity, width_here),
        "dp",
        split_axis=0,
        concat_axis=0,
        tiled=True,
    )
    source_rows = jnp.dot(
        placing.T, returned.reshape(slot_count, width_here), preferred_element_type=jnp.float32
    ).astype(jnp.bfloat16)
    partial_rows = jnp.dot(source_rows, w_out, preferred_element_type=jnp.float32)
    gained = lax.psum_scatter(partial_rows, "tensor", scatter_dimension=1, tiled=True)
    return (residual.astype(jnp.float32) + gained).astype(jnp.bfloat16)


MESH = pl.DeviceIdType.MESH
F32 = jnp.float32
BF16 = jnp.bfloat16
LANES = 128
KV_PARTS = 4
COLUMN_CHUNKS = 2


def partner_of(me, k, n):
    peer = me
    for bit in range(n.bit_length() - 1):
        flip = (k // (1 << bit)) % 2 if isinstance(k, int) else lax.rem(k // (1 << bit), 2)
        peer = peer + flip * (1 - 2 * lax.rem(me // (1 << bit), 2)) * (1 << bit)
    return peer


def iota(shape, dim):
    return lax.broadcasted_iota(jnp.int32, shape, dim)


def kernel(
    n, heads, plan, home_ref, active_ref, lengths_ref, fresh_hbm, kv_hbm, w_hbm, residual_hbm,
    out_ref,
    fresh, kv, w_mine, w_other, residual, send_q, got_q, send_i, ids, send_a, got_a, send_l, got_l,
    own, value_rows, place_back, attended, part_send, part_got, kept, gained,
    fresh_sem, kv_sem, w_sem, residual_sem, q_send, q_got, i_send, i_got, a_send, a_got, l_send,
    l_got, p_send, p_got,
):
    me = lax.axis_index("dp")
    side = lax.axis_index("tensor")
    other = 1 - side
    streams = home_ref.shape[1]
    width = heads * HD
    capacity = streams // n
    cache_len = kv.shape[2]
    columns = residual.shape[1]
    step = columns // COLUMN_CHUNKS
    scale = HD ** -0.5
    spans = [slice(h * HD, (h + 1) * HD) for h in range(heads)]
    pair = {"tensor": other}

    barrier = pltpu.get_barrier_semaphore()
    for k in range(1, n):
        pl.semaphore_signal(
            barrier, inc=1, device_id={"dp": partner_of(me, k, n)}, device_id_type=MESH
        )
    pl.semaphore_signal(barrier, inc=1, device_id=pair, device_id_type=MESH)

    fresh_copies = [
        pltpu.make_async_copy(fresh_hbm.at[i], fresh.at[i], fresh_sem.at[i]) for i in range(3)
    ]
    fresh_copies[0].start()
    part = streams // KV_PARTS
    kv_copies = [
        pltpu.make_async_copy(
            kv_hbm.at[pl.ds(i * part, part)], kv.at[pl.ds(i * part, part)], kv_sem.at[i]
        )
        for i in range(KV_PARTS)
    ]
    for copy in fresh_copies[1:] + kv_copies:
        copy.start()
    w_copies = [
        pltpu.make_async_copy(
            w_hbm.at[:, pl.ds(pl.multiple_of(at * columns, columns), columns)], dst, w_sem.at[i]
        )
        for i, (at, dst) in enumerate(((other, w_other), (side, w_mine)))
    ]
    residual_copy = pltpu.make_async_copy(residual_hbm, residual, residual_sem)

    home = home_ref[...]
    is_active = active_ref[...] > 0
    shift = streams.bit_length() - 1
    hop = lax.shift_right_logical(home, shift) ^ me
    local = (home & (streams - 1)).astype(F32)
    square = (streams, streams)
    rows_of = iota((n, streams), 0)
    sent_to = jnp.where((rows_of == hop) & is_active, 1.0, 0.0)
    before = jnp.where(iota(square, 0) < iota(square, 1), 1.0, 0.0).astype(BF16)
    rank = jnp.dot(sent_to.astype(BF16), before, preferred_element_type=F32)
    target = jnp.sum(sent_to * (rank + (rows_of * capacity).astype(F32)), axis=0, keepdims=True)
    target = jnp.where(is_active, target, -1.0)
    placing = jnp.where(iota(square, 0).astype(F32) == target, 1.0, 0.0)
    placed = placing.astype(BF16)
    slot_ids = lax.dot_general(
        jnp.broadcast_to(local, (16, streams)).astype(BF16),
        placed,
        (((1,), (1,)), ((), ())),
        preferred_element_type=F32,
    )
    send_i[...] = slot_ids[:1].astype(jnp.int32)
    fresh_copies[0].wait()
    for copy in w_copies:
        copy.start()
    residual_copy.start()
    send_q[...] = (
        jnp.dot(placed, fresh[0], preferred_element_type=F32)
        .astype(BF16)
        .reshape(n, capacity, width)
    )

    def remote(source, landing, send_sem, got_sem, k):
        return pltpu.make_async_remote_copy(
            src_ref=source,
            dst_ref=landing,
            send_sem=send_sem.at[k],
            recv_sem=got_sem.at[k],
            device_id={"dp": partner_of(me, k, n)},
            device_id_type=MESH,
        )

    def query_copy(k):
        return remote(send_q.at[k], got_q.at[k], q_send, q_got, k)

    def id_copy(k):
        return remote(send_i, ids.at[k], i_send, i_got, k)

    def back_copy(k):
        return remote(send_a.at[k], got_a.at[k], a_send, a_got, k)

    def lse_copy(k):
        return remote(send_l.at[k], got_l.at[k], l_send, l_got, k)

    query_here = pltpu.make_async_copy(send_q.at[0], got_q.at[0], q_got.at[0])
    ids_here = pltpu.make_async_copy(send_i, ids.at[0], i_got.at[0])
    back_here = pltpu.make_async_copy(send_a.at[0], got_a.at[0], a_got.at[0])
    lse_here = pltpu.make_async_copy(send_l.at[0], got_l.at[0], l_got.at[0])

    ids_here.start()
    query_here.start()
    pl.semaphore_wait(barrier, n)
    for k in range(1, n):
        id_copy(k).start()
        query_copy(k).start()

    for copy in fresh_copies[1:]:
        copy.wait()
    key_rows = jnp.dot(placed, fresh[1], preferred_element_type=F32).astype(BF16)
    value_rows[...] = jnp.dot(placed, fresh[2], preferred_element_type=F32).astype(BF16)
    lane = iota((streams, LANES), 1)
    own_scores = jnp.zeros((streams, LANES), F32)
    for h, span in enumerate(spans):
        query = send_q[:, :, span].reshape(streams, HD).astype(F32)
        key = key_rows[:, span].astype(F32)
        own_h = jnp.sum(query * key, axis=1, keepdims=True) * scale
        own_scores = jnp.where(lane == h, own_h, own_scores)
    own[...] = own_scores
    for copy in kv_copies:
        copy.wait()

    reach = (capacity, capacity * cache_len)
    offset = iota(reach, 1) - iota(reach, 0) * cache_len
    row_index = iota(reach, 0)
    eye = iota((LANES, LANES), 0) == iota((LANES, LANES), 1)

    def attend(k, carry):
        @pl.when(k == 0)
        def _():
            ids_here.wait()
            query_here.wait()

        @pl.when(k > 0)
        def _():
            id_copy(k).wait_recv()
            query_copy(k).wait_recv()

        slots = [
            jnp.clip(ids[k, 0, k * capacity + i], 0, streams - 1) for i in range(capacity)
        ]
        limit = jnp.zeros(reach, jnp.int32)
        for i, slot in enumerate(slots):
            limit = jnp.where(row_index == i, lengths_ref[0, slot], limit)
        valid = (offset >= 0) & (offset < limit)
        valid = jnp.concatenate([jnp.where(valid, 1.0, 0.0)] * heads, axis=0) > 0
        scores = jnp.concatenate(
            [
                lax.dot_general(
                    got_q[k, :, span],
                    jnp.concatenate([kv[slot, 0, :, span] for slot in slots], axis=0),
                    (((1,), (1,)), ((), ())),
                    preferred_element_type=F32,
                )
                for span in spans
            ],
            axis=0,
        )
        scores = jnp.where(valid, scores * scale, -1e30)
        top = jnp.max(scores, axis=1, keepdims=True)
        raw = jnp.exp(scores - top)
        total = jnp.sum(raw, axis=1, keepdims=True)
        weights = (raw / total).astype(BF16)
        lse = top + jnp.log(total)
        send_l[k] = jnp.sum(jnp.where(eye, lse, 0.0), axis=0, keepdims=True)
        for h, span in enumerate(spans):
            send_a[k, :, span] = jnp.dot(
                weights[h * capacity : (h + 1) * capacity],
                jnp.concatenate([kv[slot, 1, :, span] for slot in slots], axis=0),
                preferred_element_type=F32,
            ).astype(BF16)

        @pl.when(k == 0)
        def _():
            lse_here.start()
            back_here.start()

        @pl.when(k > 0)
        def _():
            lse_copy(k).start()
            back_copy(k).start()

        return carry

    def part_copy(first, last, c):
        rows = pl.ds(first * capacity, (last - first) * capacity)
        return pltpu.make_async_remote_copy(
            src_ref=part_send.at[c, rows],
            dst_ref=part_got.at[c, rows],
            send_sem=p_send.at[first, c],
            recv_sem=p_got.at[first, c],
            device_id=pair,
            device_id_type=MESH,
        )

    def project(first, last):
        rows = slice(first * capacity, last * capacity)
        for k in range(first, last):
            if k:
                back_copy(k).wait_recv()
                lse_copy(k).wait_recv()
            else:
                back_here.wait()
                lse_here.wait()
        arrived = got_a[first:last].reshape((last - first) * capacity, width)
        own_rows = own[rows]
        turned = [
            jnp.sum(jnp.where(eye, got_l[k], 0.0), axis=1, keepdims=True)
            for k in range(first, last)
        ]
        for h, span in enumerate(spans):
            lse = jnp.concatenate(
                [column[h * capacity : (h + 1) * capacity] for column in turned], axis=0
            )
            own_h = own_rows[:, h : h + 1]
            top = jnp.maximum(lse, own_h)
            from_cache = jnp.exp(lse - top)
            from_own = jnp.exp(own_h - top)
            share = 1.0 / (from_cache + from_own)
            attended[rows, span] = (
                (from_cache * share) * arrived[:, span].astype(F32)
                + (from_own * share) * value_rows[rows, span].astype(F32)
            ).astype(BF16)
        if first == 0:
            w_copies[0].wait()
        for c in range(COLUMN_CHUNKS):
            part_send[c, rows] = jnp.dot(
                attended[rows], w_other[:, c * step : (c + 1) * step], preferred_element_type=F32
            ).astype(BF16)
            part_copy(first, last, c).start()

    def keep(first, last):
        rows = slice(first * capacity, last * capacity)
        if first == 0:
            w_copies[1].wait()
        for c in range(COLUMN_CHUNKS):
            kept[c, rows] = jnp.dot(
                attended[rows], w_mine[:, c * step : (c + 1) * step], preferred_element_type=F32
            )

    def gather(first, last, c):
        rows = slice(first * capacity, last * capacity)
        for begin, end in sends:
            if first <= begin < last:
                part_copy(begin, end, c).wait()
        total = kept[c, rows] + part_got[c, rows].astype(F32)
        high = total.astype(BF16)
        gained[c, rows] = high
        gained[c, streams + first * capacity : streams + last * capacity] = (
            total - high.astype(F32)
        ).astype(BF16)

    sends = [(first, last) for what, first, last in plan if what == "project"]
    for what, first, last in plan:
        if what == "attend":
            lax.fori_loop(first, last, attend, 0)
        elif what == "project":
            project(first, last)
        else:
            keep(first, last)
    turned = jnp.transpose(placing).astype(BF16)
    place_back[...] = jnp.concatenate([turned, turned], axis=1)
    residual_copy.wait()
    late = n - n // 4
    for c in range(COLUMN_CHUNKS):
        gather(0, late, c)
    for c in range(COLUMN_CHUNKS):
        gather(late, n, c)
        span = slice(c * step, (c + 1) * step)
        out_ref[:, span] = (
            residual[:, span].astype(F32)
            + jnp.dot(place_back[...], gained[c], preferred_element_type=F32)
        ).astype(BF16)
    for k in range(1, n):
        id_copy(k).wait_send()
        query_copy(k).wait_send()
        back_copy(k).wait_send()
        lse_copy(k).wait_send()


def steps_of(n):
    q = n // 4
    return (
        ("attend", 0, 1),
        ("project", 0, 1),
        ("attend", 1, q),
        ("project", 1, 2),
        ("project", 2, q),
        ("attend", q, 2 * q),
        ("keep", 0, q),
        ("attend", 2 * q, 3 * q),
        ("project", q, q + 2),
        ("attend", 3 * q, 3 * q + 1),
        ("project", q + 2, 2 * q),
        ("attend", 3 * q + 1, 3 * q + 2),
        ("project", 2 * q, 2 * q + 2),
        ("attend", 3 * q + 2, n),
        ("project", 2 * q + 2, 3 * q),
        ("keep", q, 3 * q),
        ("project", 3 * q, 3 * q + 2),
        ("project", 3 * q + 2, n),
        ("keep", 3 * q, n),
    )


def fused_body(residual, fresh_qkv, active, home_slot, kv_cache, lengths, w_out):
    n = lax.axis_size("dp")
    streams, columns = residual.shape
    width = fresh_qkv.shape[2]
    heads = width // HD
    capacity = streams // n
    plan = steps_of(n)
    rows = (n, capacity, width)
    lse_rows = (n, 1, heads * capacity)
    step = columns // COLUMN_CHUNKS
    vmem = pl.BlockSpec(memory_space=pltpu.VMEM)
    smem = pl.BlockSpec(memory_space=pltpu.SMEM)
    anywhere = pl.BlockSpec(memory_space=pl.ANY)
    dma = pltpu.SemaphoreType.DMA
    return pl.pallas_call(
        functools.partial(kernel, n, heads, plan),
        out_shape=pltpu.VMEM((streams, columns), BF16),
        in_specs=[vmem] * 2 + [smem] + [anywhere] * 4,
        out_specs=vmem,
        scratch_shapes=[
            pltpu.VMEM((3, streams, width), BF16),
            pltpu.VMEM(kv_cache.shape, BF16),
            pltpu.VMEM((w_out.shape[0], columns), BF16),
            pltpu.VMEM((w_out.shape[0], columns), BF16),
            pltpu.VMEM(residual.shape, BF16),
            pltpu.VMEM(rows, BF16),
            pltpu.VMEM(rows, BF16),
            pltpu.VMEM((1, streams), jnp.int32),
            pltpu.SMEM((n, 1, streams), jnp.int32),
            pltpu.VMEM(rows, BF16),
            pltpu.VMEM(rows, BF16),
            pltpu.VMEM(lse_rows, F32),
            pltpu.VMEM(lse_rows, F32),
            pltpu.VMEM((streams, LANES), F32),
            pltpu.VMEM((streams, width), BF16),
            pltpu.VMEM((streams, 2 * streams), BF16),
            pltpu.VMEM((streams, width), BF16),
            pltpu.VMEM((COLUMN_CHUNKS, streams, step), BF16),
            pltpu.VMEM((COLUMN_CHUNKS, streams, step), BF16),
            pltpu.VMEM((COLUMN_CHUNKS, streams, step), F32),
            pltpu.VMEM((COLUMN_CHUNKS, 2 * streams, step), BF16),
            dma((3,)),
            dma((KV_PARTS,)),
            dma((2,)),
            dma,
        ]
        + [dma((n,))] * 8
        + [dma((n, COLUMN_CHUNKS))] * 2,
        compiler_params=pltpu.CompilerParams(
            collective_id=0, has_side_effects=True, vmem_limit_bytes=60 * 1024 * 1024
        ),
    )(
        home_slot.reshape(1, streams),
        active.reshape(1, streams),
        lengths.reshape(1, streams),
        jnp.transpose(fresh_qkv, (1, 0, 2)),
        kv_cache,
        w_out,
        residual,
    )


def body(residual, fresh_qkv, active, home_slot, kv_cache, lengths, w_out):
    n = lax.axis_size("dp")
    streams = home_slot.shape[0]
    heads = fresh_qkv.shape[2] // HD
    fits = (
        lax.axis_size("tensor") == 2
        and n % 16 == 0
        and n & (n - 1) == 0
        and streams == 16 * n
        and streams <= 256
        and heads * 16 == LANES
        and kv_cache.shape[2] == 16
    )
    chosen = fused_body if fits else general_body
    return chosen(residual, fresh_qkv, active, home_slot, kv_cache, lengths, w_out)


def solution(mesh):
    placed = (
        P("dp", "tensor"),
        P("dp", None, "tensor"),
        P("dp"),
        P("dp"),
        P("dp", None, None, "tensor"),
        P("dp"),
        P("tensor", None),
    )
    return jax.shard_map(
        body, mesh=mesh, in_specs=placed, out_specs=P("dp", "tensor"), check_vma=False
    )
```
